32 devices in a mesh: groups: 2 (over y), seq: 4 (over z), head: 2 (over x), rep: 2 (over core).
Axes of the slice: x: 2, y: 2, z: 4, core: 2. Of those that a mesh axis runs over, the one named last changes fastest.
Arguments:
- queries: bfloat16 [2048, 6144], P(('groups', 'seq', 'rep'), 'head'), parts along dimension 0, may hold values from -150 to 150
- key_tokens: bfloat16 [2048, 6144], P(('groups', 'seq', 'rep'), 'head'), parts along dimension 0, may hold values from -6 to 6
- value_tokens: bfloat16 [2048, 6144], P(('groups', 'seq', 'rep'), 'head'), parts along dimension 0, may hold values from -6 to 6
- stream: bfloat16 [2048, 6144], P(('groups', 'seq', 'rep'), 'head'), parts along dimension 0, may hold values from -6 to 6
- norm_gain: float32 [6144], P('head'), may hold values from 0.1 to 1.9
- latent_weight: bfloat16 [6144, 64], P('head'), may hold values from -0.078125 to 0.078125
- tile_pool: bfloat16 [8, 64, 2, 128], P(('groups', 'seq')), parts along dimension 0, may hold values from -6 to 6
- tile_position: int32 [8], P('groups'), parts along dimension 0, may hold values from 0 to 3, each once
- lift_weight: bfloat16 [64, 512], P(None, ('head', 'rep')), may hold values from -0.75 to 0.75
- lift_bias: float32 [512], P(('head', 'rep')), may hold values from -3 to 3
- conv_weight: bfloat16 [2, 27, 512, 512], P(None, None, ('head', 'rep')), may hold values from -0.0546875 to 0.0546875
Outputs:
- hidden: bfloat16 [2048, 6144], P(('groups', 'seq', 'rep'), 'head'), parts along dimension 0
- latents: float32 [2048, 64], P(('groups', 'seq', 'rep')), parts along dimension 0
- decoded: float32 [1024, 2, 4, 128], P(('groups', 'head', 'rep'), None, 'seq'), parts along dimension 0
The draws below stay inside these ranges and needn't reach their ends.
There are 2 independent parts, one for each index of `groups`. The reference program is written for one: setup_inputs(seed, part) draws one part's arguments, and reference() takes and returns one part's arrays. A program takes and returns all parts, laid end to end along the dimension named above; an argument that names none is the same for every part. Nothing has to cross between parts.
Inputs may be any that keep to these rules, and one draw needn't show every extreme that they name: `tile_position`: each of the 4 grid rows is named by exactly one pool tile.
All inputs are finite; a program needn't handle non-finite values.
Results may differ from the reference program's by a relative error of at most 0.01.
Values may be sent and summed in bfloat16 or wider, within the bound.
A program may use at most 128 MiB of HBM per device.

```python
import math
import jax
import jax.numpy as jnp
from jax import lax

HEADS = 48
HEAD_DIM = 128
WIDTH = 6144
LATENT = 64
CHANNELS = 512
FRAMES = 2
COLS = 128
DLAYERS = 2
TOKENS = 1024
TILES = 4


def key_draw(key):
    return jnp.clip(jax.random.normal(jax.random.fold_in(key, 102), (TOKENS, WIDTH), jnp.float32), -6.0, 6.0)


def draw_key_tokens(key, part):
    drawn = key_draw(key)
    return drawn.astype(jnp.bfloat16)


def draw_queries(key, part):
    drawn = jnp.clip(2.5 * jax.random.normal(jax.random.fold_in(key, 104), (TOKENS, WIDTH), jnp.float32), -15.0, 15.0)
    return drawn.astype(jnp.bfloat16)


def block_scale(stream_key, extent, pieces, smallest, largest):
    loudness = 1.0
    for axis_at, shards_of in pieces:
        steps = jax.random.uniform(jax.random.fold_in(jax.random.fold_in(stream_key, 6), axis_at), (shards_of,), jnp.float32, smallest / len(pieces), largest / len(pieces))
        loudness = loudness * jnp.repeat(jnp.exp(steps), extent[axis_at] // shards_of).reshape((-1,) + (1,) * (len(extent) - 1 - axis_at))
    return loudness


def noise(own_key, extent, spread, limit, cuts=(), kind=jnp.bfloat16):
    entries = spread * jax.random.normal(own_key, extent, jnp.float32)
    if cuts:
        entries = entries * block_scale(own_key, extent, cuts, -0.22, 0.18)
    return jnp.clip(entries, -limit, limit).astype(kind)


def setup_inputs(seed: int = 0, part: int = 0) -> dict:
    key_of = jax.random.split(jax.random.key(seed), 12)
    own_keys = jax.random.split(jax.random.fold_in(key_of[11], part), 12)
    queries = draw_queries(jax.random.fold_in(jax.random.fold_in(key_of[11], part), 71), part)
    key_tokens = draw_key_tokens(jax.random.fold_in(jax.random.fold_in(key_of[11], part), 71), part)
    value_tokens = noise(own_keys[2], (TOKENS, WIDTH), 1.0, 6.0, ((0, 8), (1, 2)))
    stream = noise(own_keys[3], (TOKENS, WIDTH), 1.0, 6.0, ((0, 8), (1, 2)))
    norm_gain = jnp.clip(1.0 + 0.18 * jax.random.normal(key_of[4], (WIDTH,), jnp.float32), 0.1, 1.9)
    latent_weight = noise(key_of[5], (WIDTH, LATENT), WIDTH ** -0.5, 0.078125, ((0, 2),))
    tile_pool = noise(own_keys[6], (TILES, LATENT, FRAMES, COLS), 1.0, 6.0, ((0, 4),))
    tile_position = jax.random.permutation(own_keys[7], TILES).astype(jnp.int32)
    lift_weight = noise(key_of[8], (LATENT, CHANNELS), LATENT ** -0.5, 0.75, ((1, 4),))
    lift_bias = noise(key_of[9], (CHANNELS,), 0.5, 3.0, ((0, 4),), jnp.float32)
    conv_weight = noise(key_of[10], (DLAYERS, 27, CHANNELS, CHANNELS), (27 * CHANNELS) ** -0.5, 0.0546875, ((2, 4),))
    return {"queries": queries, "key_tokens": key_tokens, "value_tokens": value_tokens, "stream": stream, "norm_gain": norm_gain, "latent_weight": latent_weight, "tile_pool": tile_pool, "tile_position": tile_position, "lift_weight": lift_weight, "lift_bias": lift_bias, "conv_weight": conv_weight}


epsilon = 1e-06

def head_attention(operands):
    query_head, key_head, value_head = operands
    scores = jnp.dot(query_head, key_head.T, preferred_element_type=jnp.float32) * (1.0 / math.sqrt(HEAD_DIM))
    row_peak = lax.optimization_barrier(jnp.max(scores, axis=1, keepdims=True))
    exponent = jnp.exp(scores - row_peak)
    weights = exponent.astype(jnp.bfloat16)
    summed = jnp.dot(weights, value_head, preferred_element_type=jnp.float32)
    return (summed / lax.optimization_barrier(jnp.sum(exponent, axis=1, keepdims=True))).astype(jnp.bfloat16)

def by_heads(matrix):
    return jnp.transpose(matrix.reshape(TOKENS, HEADS, HEAD_DIM), (1, 0, 2))

def reference(queries, key_tokens, value_tokens, stream, norm_gain, latent_weight, tile_pool, tile_position, lift_weight, lift_bias, conv_weight):
    attended = lax.map(head_attention, (by_heads(queries), by_heads(key_tokens), by_heads(value_tokens)))
    attended = jnp.transpose(attended, (1, 0, 2)).reshape(TOKENS, WIDTH)
    hidden = (stream.astype(jnp.float32) + attended.astype(jnp.float32)).astype(jnp.bfloat16)
    widened = hidden.astype(jnp.float32)
    scaled = (widened * norm_gain).astype(jnp.bfloat16)
    projected = jnp.dot(scaled, latent_weight, preferred_element_type=jnp.float32)
    squares = lax.optimization_barrier(jnp.sum(widened * widened, axis=1))
    latents = projected * lax.rsqrt(squares / WIDTH + epsilon)[:, None]
    latent_grid = jnp.zeros((LATENT, FRAMES, TILES, COLS), jnp.bfloat16)
    latent_grid = latent_grid.at[:, :, tile_position.astype(jnp.int32), :].set(jnp.transpose(tile_pool, (1, 2, 0, 3)))
    feature_map = jnp.dot(lift_weight.T, latent_grid.reshape(LATENT, -1), preferred_element_type=jnp.float32) + lift_bias[:, None]
    for layer_index in range(DLAYERS):
        active = jax.nn.silu(feature_map).astype(jnp.bfloat16).reshape(CHANNELS, FRAMES, TILES, COLS)
        padded = jnp.pad(active, ((0, 0), (1, 1), (1, 1), (1, 1)))
        update = jnp.zeros((CHANNELS, FRAMES * TILES * COLS), jnp.float32)
        for frame_off in range(3):
            for row_off in range(3):
                for col_off in range(3):
                    window = padded[:, frame_off:frame_off + FRAMES, row_off:row_off + TILES, col_off:col_off + COLS].reshape(CHANNELS, -1)
                    tap_weight = conv_weight[layer_index, frame_off * 9 + row_off * 3 + col_off]
                    update = update + lax.dot_general(tap_weight, window, (((1,), (0,)), ((), ())), preferred_element_type=jnp.float32)
        feature_map = feature_map + update
    decoded = feature_map.reshape(CHANNELS, FRAMES, TILES, COLS)
    return (hidden, latents, decoded)
```

```python
import functools
import math

import jax
import jax.numpy as jnp
from jax import lax
from jax.experimental import pallas as pl
from jax.experimental.pallas import tpu as pltpu
from jax.sharding import PartitionSpec as P

HEAD_DIM = 128
WIDTH = 6144


epsilon = 1e-06
negative = -1e30


def padded(shard, sides, width):
    for axis, dim in sides:
        peers, length = (lax.axis_size(axis), shard.shape[dim])
        up = [(i, (i + 1) % peers) for i in range(peers - 1)]
        down = [(j, i) for i, j in up]
        last = lax.slice_in_dim(shard, length - width, length, axis=dim)
        leading = lax.slice_in_dim(shard, 0, width, axis=dim)
        before = lax.ppermute(last, axis, up)
        after = lax.ppermute(leading, axis, down)
        shard = jnp.concatenate([before, shard, after], axis=dim)
    return shard


def prepare(block_rows):
    row_count = block_rows.shape[0]
    head_count = block_rows.shape[1] // HEAD_DIM
    query_heads = block_rows.reshape(row_count, head_count, HEAD_DIM)
    initial = (
        jnp.full((head_count, row_count), negative, jnp.float32),
        jnp.zeros((head_count, row_count), jnp.float32),
        jnp.zeros((head_count, row_count, HEAD_DIM), jnp.float32),
    )
    return (query_heads, initial)


def make_update(query_heads, state, pieces):
    head_count = query_heads.shape[1]
    factor = 1.0 / math.sqrt(HEAD_DIM)
    running_max, running_sum, accum = state
    key_piece, value_piece = pieces
    piece_rows = key_piece.shape[0]
    key_heads = key_piece.reshape(piece_rows, head_count, HEAD_DIM)
    value_heads = value_piece.reshape(piece_rows, head_count, HEAD_DIM)
    scores = (
        jnp.einsum("qhd,khd->hqk", query_heads, key_heads, preferred_element_type=jnp.float32)
        * factor
    )
    new_max = jnp.maximum(running_max, jnp.max(scores, axis=2))
    exponent = jnp.exp(scores - new_max[:, :, None])
    running_sum = jnp.sum(exponent, axis=2)
    accum = jnp.einsum(
        "hqk,khd->hqd",
        exponent.astype(jnp.bfloat16),
        value_heads,
        preferred_element_type=jnp.float32,
    )
    return (new_max, running_sum, accum)


def finish(state):
    running_max, running_sum, accum = state
    result = accum / running_sum[:, :, None]
    return jnp.transpose(result, (1, 0, 2)).reshape(result.shape[1], -1).astype(jnp.bfloat16)


def shift_columns(window, col_shift):
    if col_shift == 0:
        return window
    edge = jnp.zeros(window.shape[:-1] + (1,), window.dtype)
    if col_shift < 0:
        return jnp.concatenate([edge, window[..., :-1]], axis=-1)
    return jnp.concatenate([window[..., 1:], edge], axis=-1)


def tap_sum(running, piece_block, layer_weight):
    piece_rows = piece_block.shape[0]
    frames = piece_block.shape[1]
    band_rows = piece_block.shape[2] - 2
    framed = jnp.pad(piece_block, ((0, 0), (1, 1), (0, 0), (0, 0)))
    for frame_off in range(3):
        for row_off in range(3):
            for col_off in range(3):
                window = shift_columns(
                    framed[:, frame_off : frame_off + frames, row_off : row_off + band_rows, :],
                    col_off - 1,
                )
                tap_weight = layer_weight[frame_off * 9 + row_off * 3 + col_off]
                running = running + lax.dot_general(
                    tap_weight,
                    window.reshape(piece_rows, -1),
                    (((1,), (0,)), ((), ())),
                    preferred_element_type=jnp.float32,
                )
    return running


def make_pick(tile_position, own_rows, piece_block):
    selector = (own_rows[:, None] == tile_position[None, :]).astype(jnp.bfloat16)
    return jnp.einsum("tp,plfc->lftc", selector, piece_block, preferred_element_type=jnp.float32)


MESH = pl.DeviceIdType.MESH


def fused_kernel(
    seq_size, rep_size, head_size,
    q_ref, k_ref, v_ref, stream_ref, gain_ref, lw_ref,
    hid_ref, lat_ref,
    qkv, obuf, att, part, part_in,
    send_sem, recv_sem, osend_sem, orecv_sem, psend_sem, precv_sem,
):
    seq, rep, head = (lax.axis_index(a) for a in ("seq", "rep", "head"))
    count = seq_size * rep_size
    me = seq * rep_size + rep
    rows = q_ref.shape[0]
    own_heads = qkv.shape[0]
    others = count - 1
    factor = 1.0 / math.sqrt(HEAD_DIM)
    offsets = [(d, e) for d in (2, 1, 3, 0) for e in range(rep_size) if (d, e) != (0, 0)]

    def peer(d, e):
        return lax.rem(seq + d, seq_size), lax.rem(rep + e, rep_size)

    partner = {"head": lax.rem(head + 1, head_size)}
    barrier = pltpu.get_barrier_semaphore()
    for d, e in offsets:
        ps, pr = peer(d, e)
        pl.semaphore_signal(barrier, inc=1, device_id={"seq": ps, "rep": pr}, device_id_type=MESH)
    pl.semaphore_signal(barrier, inc=1, device_id=partner, device_id_type=MESH)
    pl.semaphore_wait(barrier, others + 1)

    my_rows = pl.ds(pl.multiple_of(me * rows, rows), rows)
    sources = (q_ref, k_ref, v_ref)
    for h in range(own_heads):
        for d, e in offsets:
            ps, pr = peer(d, e)
            column = ((ps * rep_size + pr) * own_heads + h) * HEAD_DIM
            columns = pl.ds(pl.multiple_of(column, HEAD_DIM), HEAD_DIM)
            for a, source in enumerate(sources):
                pltpu.make_async_remote_copy(
                    src_ref=source.at[:, columns],
                    dst_ref=qkv.at[h, a, my_rows, :],
                    send_sem=send_sem,
                    recv_sem=recv_sem.at[h],
                    device_id={"seq": ps, "rep": pr},
                    device_id_type=MESH,
                ).start()
    for h in range(own_heads):
        columns = pl.ds(pl.multiple_of((me * own_heads + h) * HEAD_DIM, HEAD_DIM), HEAD_DIM)
        for a, source in enumerate(sources):
            qkv[h, a, my_rows, :] = source[:, columns]

    def arrived(ref, sem):
        pltpu.make_async_copy(ref, ref, sem).wait()

    block = rep_size * rows
    for h in range(own_heads):
        arrived(qkv.at[h, :, pl.ds(0, others * rows), :], recv_sem.at[h])
        out_columns = pl.ds(pl.multiple_of((me * own_heads + h) * HEAD_DIM, HEAD_DIM), HEAD_DIM)

        def attend(step, carry):
            target = lax.rem(seq + 2 + step, seq_size)
            here = pl.ds(pl.multiple_of(target * block, block), block)
            scores = lax.dot_general(
                qkv[h, 0, here, :], qkv[h, 1], (((1,), (1,)), ((), ())),
                preferred_element_type=jnp.float32,
            ) * factor
            exponent = jnp.exp(scores - jnp.max(scores, axis=1, keepdims=True))
            total = jnp.sum(exponent, axis=1, keepdims=True)
            summed = jnp.dot(
                exponent.astype(jnp.bfloat16), qkv[h, 2], preferred_element_type=jnp.float32
            )
            obuf[h, here, :] = (summed / total).astype(jnp.bfloat16)
            for r in range(rep_size):
                @pl.when(jnp.logical_or(target != seq, rep != r))
                def _():
                    start = pl.multiple_of(target * block + r * rows, rows)
                    pltpu.make_async_remote_copy(
                        src_ref=obuf.at[h, pl.ds(start, rows), :],
                        dst_ref=att.at[:, out_columns],
                        send_sem=osend_sem,
                        recv_sem=orecv_sem.at[h],
                        device_id={"seq": target, "rep": r},
                        device_id_type=MESH,
                    ).start()
            return carry

        lax.fori_loop(0, seq_size, attend, 0)
        att[:, out_columns] = obuf[h, my_rows, :]

    squares = jnp.zeros((rows, HEAD_DIM), jnp.float32)
    projected = jnp.zeros((rows, lw_ref.shape[0]), jnp.float32)
    for h in range(own_heads):
        arrived(obuf.at[h, pl.ds(0, others * rows), :], orecv_sem.at[h])
        for j in range(count):
            low = (j * own_heads + h) * HEAD_DIM
            cols = slice(low, low + HEAD_DIM)
            combined = stream_ref[:, cols].astype(jnp.float32) + att[:, cols].astype(jnp.float32)
            hidden = combined.astype(jnp.bfloat16)
            hid_ref[:, cols] = hidden
            widened = hidden.astype(jnp.float32)
            squares = squares + widened * widened
            scaled = (widened * gain_ref[:, cols]).astype(jnp.bfloat16)
            projected = projected + lax.dot_general(
                scaled, lw_ref[:, cols], (((1,), (1,)), ((), ())),
                preferred_element_type=jnp.float32,
            )
    latent = projected.shape[1]
    summed = jnp.sum(squares, axis=1, keepdims=True)
    part[:, :latent] = projected
    part[:, latent:] = jnp.broadcast_to(summed, (rows, part.shape[1] - latent))
    swap = pltpu.make_async_remote_copy(
        src_ref=part, dst_ref=part_in, send_sem=psend_sem, recv_sem=precv_sem,
        device_id=partner, device_id_type=MESH,
    )
    swap.start()
    arrived(qkv.at[:, :, pl.ds(0, others * rows), :], send_sem)
    arrived(obuf.at[:, pl.ds(0, others * rows), :], osend_sem)
    swap.wait()
    both = part[...] + part_in[...]
    width = q_ref.shape[1] * head_size
    lat_ref[...] = both[:, :latent] * lax.rsqrt(both[:, latent:latent + 1] / width + epsilon)


def fused(queries, key_tokens, value_tokens, stream, norm_gain, latent_weight):
    seq_size, rep_size, head_size = (lax.axis_size(a) for a in ("seq", "rep", "head"))
    rows, width = queries.shape
    count = seq_size * rep_size
    own_heads = width // HEAD_DIM // count
    latent = latent_weight.shape[1]
    lanes = 2 * latent
    bf = jnp.bfloat16
    vmem = pl.BlockSpec(memory_space=pltpu.VMEM)
    dma = pltpu.SemaphoreType.DMA
    return pl.pallas_call(
        functools.partial(fused_kernel, seq_size, rep_size, head_size),
        out_shape=(
            jax.ShapeDtypeStruct((rows, width), bf),
            jax.ShapeDtypeStruct((rows, latent), jnp.float32),
        ),
        in_specs=[vmem] * 6,
        out_specs=(vmem, vmem),
        scratch_shapes=[
            pltpu.VMEM((own_heads, 3, count * rows, HEAD_DIM), bf),
            pltpu.VMEM((own_heads, count * rows, HEAD_DIM), bf),
            pltpu.VMEM((rows, width), bf),
            pltpu.VMEM((rows, lanes), jnp.float32),
            pltpu.VMEM((rows, lanes), jnp.float32),
            dma, dma((own_heads,)), dma, dma((own_heads,)), dma, dma,
        ],
        compiler_params=pltpu.CompilerParams(
            collective_id=0, has_side_effects=True, vmem_limit_bytes=48 << 20
        ),
    )(queries, key_tokens, value_tokens, stream, norm_gain[None, :], latent_weight.T)


def gathered(queries, key_tokens, value_tokens, stream, norm_gain, latent_weight):
    query_heads, initial = prepare(queries)
    state = make_update(
        query_heads,
        initial,
        (
            lax.all_gather(key_tokens, ("seq", "rep"), axis=0, tiled=True),
            lax.all_gather(value_tokens, ("seq", "rep"), axis=0, tiled=True),
        ),
    )
    attended = finish(state)
    combined = stream.astype(jnp.float32) + attended.astype(jnp.float32)
    hidden = combined.astype(jnp.bfloat16)
    widened = hidden.astype(jnp.float32)
    scaled = (widened * norm_gain).astype(jnp.bfloat16)
    partial_proj = jnp.dot(scaled, latent_weight, preferred_element_type=jnp.float32)
    partial_squares = jnp.sum(widened * widened, axis=1)
    projected, squares = (
        lax.psum(partial_proj.astype(jnp.bfloat16), "head").astype(jnp.float32),
        lax.psum(partial_squares.astype(jnp.bfloat16), "head").astype(jnp.float32),
    )
    latents = projected * lax.rsqrt(squares / WIDTH + epsilon)[:, None]
    return hidden, latents


def shards(
    queries,
    key_tokens,
    value_tokens,
    stream,
    norm_gain,
    latent_weight,
    tile_pool,
    tile_position,
    lift_weight,
    lift_bias,
    conv_weight,
):
    heads_here = queries.shape[1] // HEAD_DIM
    spread = lax.axis_size("seq") * lax.axis_size("rep")
    fits = heads_here % spread == 0 and lax.axis_size("seq") == 4 and lax.axis_size("head") == 2
    attention = fused if fits else gathered
    hidden, latents = attention(
        queries, key_tokens, value_tokens, stream, norm_gain, latent_weight
    )
    tiles_here = tile_pool.shape[0]
    frames = tile_pool.shape[2]
    columns = tile_pool.shape[3]
    own_rows = lax.axis_index("seq") * tiles_here + jnp.arange(tiles_here, dtype=jnp.int32)
    collected = make_pick(
        tile_position, own_rows, lax.all_gather(tile_pool, "seq", axis=0, tiled=True)
    )
    latent_grid = collected.astype(jnp.bfloat16)
    channels_here = lift_weight.shape[1]
    feature_map = (
        lax.dot_general(
            lift_weight,
            latent_grid.reshape(latent_grid.shape[0], -1),
            (((0,), (0,)), ((), ())),
            preferred_element_type=jnp.float32,
        )
        + lift_bias[:, None]
    )
    for layer_index in range(conv_weight.shape[0]):
        layer_weight = conv_weight[layer_index]
        active = (
            jax.nn.silu(feature_map)
            .astype(jnp.bfloat16)
            .reshape(channels_here, frames, tiles_here, columns)
        )
        zeros_here = jnp.zeros(feature_map.shape, jnp.float32)
        bordered = padded(active, (("seq", 2),), 1)
        rimmed = lax.all_gather(bordered, ("head", "rep"), axis=0, tiled=True)
        update = tap_sum(zeros_here, rimmed, layer_weight)
        feature_map = feature_map + update
    decoded = feature_map.reshape(channels_here, frames, tiles_here, columns)
    return (hidden, latents, decoded)


def solution(mesh):
    in_specs = (
        P(("groups", "seq", "rep"), "head"),
        P(("groups", "seq", "rep"), "head"),
        P(("groups", "seq", "rep"), "head"),
        P(("groups", "seq", "rep"), "head"),
        P("head"),
        P("head", None),
        P(("groups", "seq"), None, None, None),
        P("groups"),
        P(None, ("head", "rep")),
        P(("head", "rep")),
        P(None, None, ("head", "rep"), None),
    )
    out_specs = (
        P(("groups", "seq", "rep"), "head"),
        P(("groups", "seq", "rep"), None),
        P(("groups", "head", "rep"), None, "seq", None),
    )
    return jax.shard_map(shards, mesh=mesh, in_specs=in_specs, out_specs=out_specs, check_vma=False)
```

```python
import functools
import math

import jax
import jax.numpy as jnp
from jax import lax
from jax.experimental import pallas as pl
from jax.experimental.pallas import tpu as pltpu
from jax.sharding import PartitionSpec as P

HEAD_DIM = 128
WIDTH = 6144


epsilon = 1e-06
negative = -1e30


def padded(shard, sides, width):
    for axis, dim in sides:
        peers, length = (lax.axis_size(axis), shard.shape[dim])
        up = [(i, (i + 1) % peers) for i in range(peers - 1)]
        down = [(j, i) for i, j in up]
        last = lax.slice_in_dim(shard, length - width, length, axis=dim)
        leading = lax.slice_in_dim(shard, 0, width, axis=dim)
        before = lax.ppermute(last, axis, up)
        after = lax.ppermute(leading, axis, down)
        shard = jnp.concatenate([before, shard, after], axis=dim)
    return shard


def prepare(block_rows):
    row_count = block_rows.shape[0]
    head_count = block_rows.shape[1] // HEAD_DIM
    query_heads = block_rows.reshape(row_count, head_count, HEAD_DIM)
    initial = (
        jnp.full((head_count, row_count), negative, jnp.float32),
        jnp.zeros((head_count, row_count), jnp.float32),
        jnp.zeros((head_count, row_count, HEAD_DIM), jnp.float32),
    )
    return (query_heads, initial)


def make_update(query_heads, state, pieces):
    head_count = query_heads.shape[1]
    factor = 1.0 / math.sqrt(HEAD_DIM)
    running_max, running_sum, accum = state
    key_piece, value_piece = pieces
    piece_rows = key_piece.shape[0]
    key_heads = key_piece.reshape(piece_rows, head_count, HEAD_DIM)
    value_heads = value_piece.reshape(piece_rows, head_count, HEAD_DIM)
    scores = (
        jnp.einsum("qhd,khd->hqk", query_heads, key_heads, preferred_element_type=jnp.float32)
        * factor
    )
    new_max = jnp.maximum(running_max, jnp.max(scores, axis=2))
    exponent = jnp.exp(scores - new_max[:, :, None])
    running_sum = jnp.sum(exponent, axis=2)
    accum = jnp.einsum(
        "hqk,khd->hqd",
        exponent.astype(jnp.bfloat16),
        value_heads,
        preferred_element_type=jnp.float32,
    )
    return (new_max, running_sum, accum)


def finish(state):
    running_max, running_sum, accum = state
    result = accum / running_sum[:, :, None]
    return jnp.transpose(result, (1, 0, 2)).reshape(result.shape[1], -1).astype(jnp.bfloat16)


def shift_columns(window, col_shift):
    if col_shift == 0:
        return window
    edge = jnp.zeros(window.shape[:-1] + (1,), window.dtype)
    if col_shift < 0:
        return jnp.concatenate([edge, window[..., :-1]], axis=-1)
    return jnp.concatenate([window[..., 1:], edge], axis=-1)


def tap_sum(running, piece_block, layer_weight):
    piece_rows = piece_block.shape[0]
    frames = piece_block.shape[1]
    band_rows = piece_block.shape[2] - 2
    framed = jnp.pad(piece_block, ((0, 0), (1, 1), (0, 0), (0, 0)))
    for frame_off in range(3):
        for row_off in range(3):
            for col_off in range(3):
                window = shift_columns(
                    framed[:, frame_off : frame_off + frames, row_off : row_off + band_rows, :],
                    col_off - 1,
                )
                tap_weight = layer_weight[frame_off * 9 + row_off * 3 + col_off]
                running = running + lax.dot_general(
                    tap_weight,
                    window.reshape(piece_rows, -1),
                    (((1,), (0,)), ((), ())),
                    preferred_element_type=jnp.float32,
                )
    return running


def make_pick(tile_position, own_rows, piece_block):
    selector = (own_rows[:, None] == tile_position[None, :]).astype(jnp.bfloat16)
    return jnp.einsum("tp,plfc->lftc", selector, piece_block, preferred_element_type=jnp.float32)


MESH = pl.DeviceIdType.MESH


def fused_kernel(
    seq_size, rep_size, head_size,
    q_ref, k_ref, v_ref, stream_ref, gain_ref, lw_ref,
    tile_ref, pick_ref, lift_ref, bias_ref, conv_ref,
    hid_ref, lat_ref, dec_ref,
    qkv, obuf, att, part, part_in,
    tiles, lifts, biases, taps, act1, act2, feat, acc,
    send_sem, recv_sem, osend_sem, orecv_sem, psend_sem, precv_sem,
    tap_sem, dsend_sem, drecv_sem,
):
    seq, rep, head = (lax.axis_index(a) for a in ("seq", "rep", "head"))
    count = seq_size * rep_size
    me = seq * rep_size + rep
    rows = q_ref.shape[0]
    own_heads = qkv.shape[0]
    others = count - 1
    factor = 1.0 / math.sqrt(HEAD_DIM)
    offsets = [(d, e) for d in (2, 1, 3, 0) for e in range(rep_size) if (d, e) != (0, 0)]

    def peer(d, e):
        return lax.rem(seq + d, seq_size), lax.rem(rep + e, rep_size)

    partner = {"head": lax.rem(head + 1, head_size)}
    mates = [
        {"head": lax.rem(head + d, head_size), "rep": lax.rem(rep + e, rep_size)}
        for d in range(head_size) for e in range(rep_size) if (d, e) != (0, 0)
    ]
    quarter = head * rep_size + rep
    tap_copy = pltpu.make_async_copy(conv_ref, taps, tap_sem)
    tap_copy.start()
    barrier = pltpu.get_barrier_semaphore()
    for d, e in offsets:
        ps, pr = peer(d, e)
        pl.semaphore_signal(barrier, inc=1, device_id={"seq": ps, "rep": pr}, device_id_type=MESH)
    strangers = [m for m, e in zip(mates, range(1, head_size * rep_size)) if e >= rep_size]
    for mate in strangers:
        pl.semaphore_signal(barrier, inc=1, device_id=mate, device_id_type=MESH)
    pl.semaphore_wait(barrier, others + len(strangers))

    def arrived(ref, sem):
        pltpu.make_async_copy(ref, ref, sem).wait()

    def send(source, target, index, device):
        pltpu.make_async_remote_copy(
            src_ref=source, dst_ref=target,
            send_sem=dsend_sem.at[index], recv_sem=drecv_sem.at[index],
            device_id=device, device_id_type=MESH,
        ).start()

    share = tile_ref.shape[0] // (head_size * rep_size)
    my_share = pl.ds(pl.multiple_of(quarter * share, share), share)
    for d in range(1, seq_size):
        send(tile_ref.at[my_share, :], tiles.at[seq, my_share, :], 0,
             {"seq": lax.rem(seq + d, seq_size)})
    for mate in mates:
        send(lift_ref, lifts.at[quarter], 1, mate)
        send(bias_ref, biases.at[quarter], 2, mate)

    my_rows = pl.ds(pl.multiple_of(me * rows, rows), rows)
    sources = (q_ref, k_ref, v_ref)
    for h in range(own_heads):
        for d, e in offsets:
            ps, pr = peer(d, e)
            column = ((ps * rep_size + pr) * own_heads + h) * HEAD_DIM
            columns = pl.ds(pl.multiple_of(column, HEAD_DIM), HEAD_DIM)
            for a, source in enumerate(sources):
                pltpu.make_async_remote_copy(
                    src_ref=source.at[:, columns],
                    dst_ref=qkv.at[h, a, my_rows, :],
                    send_sem=send_sem,
                    recv_sem=recv_sem.at[h],
                    device_id={"seq": ps, "rep": pr},
                    device_id_type=MESH,
                ).start()
    for h in range(own_heads):
        columns = pl.ds(pl.multiple_of((me * own_heads + h) * HEAD_DIM, HEAD_DIM), HEAD_DIM)
        for a, source in enumerate(sources):
            qkv[h, a, my_rows, :] = source[:, columns]

    tiles[seq, my_share, :] = tile_ref[my_share, :]
    lifts[quarter] = lift_ref[...]
    biases[quarter] = bias_ref[...]
    pieces = len(mates)
    arrived(tiles.at[pl.ds(0, seq_size - 1), pl.ds(0, share), :], drecv_sem.at[0])
    for mate in mates:
        send(tiles.at[:, my_share, :], tiles.at[:, my_share, :], 3, mate)
    arrived(lifts.at[pl.ds(0, pieces)], drecv_sem.at[1])
    arrived(biases.at[pl.ds(0, pieces)], drecv_sem.at[2])
    arrived(tiles.at[:, pl.ds(0, pieces * share), :], drecv_sem.at[3])

    frames, reach, columns_here, channels = act1.shape
    own = lift_ref.shape[1]
    margin = reach // 2
    own_lanes = pl.ds(pl.multiple_of(quarter * own, own), own)

    def inside(d):
        row = seq + d
        return jnp.where(jnp.logical_and(row >= 0, row < seq_size), 1.0, 0.0)

    def silu(value):
        return value / (1.0 + jnp.exp(-value))

    def lifted(chosen, weight, bias):
        return lax.dot_general(
            chosen, weight, (((0,), (0,)), ((), ())), preferred_element_type=jnp.float32
        ) + bias

    for d in range(reach):
        chosen = jnp.zeros(tile_ref.shape, jnp.float32)
        for p in range(seq_size):
            chosen = chosen + pick_ref[d, p] * tiles[p].astype(jnp.float32)
        chosen = chosen.astype(jnp.bfloat16)
        for c in range(pieces + 1):
            active = silu(lifted(chosen, lifts[c], biases[c, :1, :])) * inside(d - margin)
            act1[:, d, :, c * own:(c + 1) * own] = active.astype(jnp.bfloat16).reshape(
                frames, columns_here, own
            )
        if 1 <= d <= reach - 2:
            feat[:, d - 1] = lifted(chosen, lift_ref[...], bias_ref[:1, :]).reshape(
                frames, columns_here, own
            )

    def convolve(layer, active, rows_out):
        length = rows_out * columns_here
        for f in range(frames):
            first = True
            for a in range(3):
                if not 0 <= f + a - 1 < frames:
                    continue
                for b in range(3):
                    window = active[f + a - 1, b:b + rows_out].reshape(length, channels)
                    base = 9 * a + 3 * b
                    term = lax.dot_general(
                        window, taps[layer, base:base + 3].reshape(3 * own, channels),
                        (((1,), (1,)), ((), ())), preferred_element_type=jnp.float32,
                    )
                    acc[f, :length, :] = term if first else acc[f, :length, :] + term
                    first = False

    def gathered_columns(f, r):
        lines = slice(r * columns_here, (r + 1) * columns_here)
        at = lax.broadcasted_iota(jnp.int32, (columns_here, own), 0)
        before = pltpu.roll(acc[f, lines, :own], 1, 0)
        after = pltpu.roll(acc[f, lines, 2 * own:], columns_here - 1, 0)
        return (
            acc[f, lines, own:2 * own]
            + jnp.where(at == 0, 0.0, before)
            + jnp.where(at == columns_here - 1, 0.0, after)
        )

    tap_copy.wait()
    convolve(0, act1, reach - 2)
    for f in range(frames):
        for r in range(reach - 2):
            value = feat[f, r] + gathered_columns(f, r)
            feat[f, r] = value
            act2[f, r, :, own_lanes] = (silu(value) * inside(r + 1 - margin)).astype(jnp.bfloat16)
    for mate in mates:
        send(act2.at[:, :, :, own_lanes], act2.at[:, :, :, own_lanes], 4, mate)

    def last_layer():
        arrived(act2.at[:, :, :, pl.ds(0, pieces * own)], drecv_sem.at[4])
        convolve(1, act2, reach - 4)
        for f in range(frames):
            dec_ref[f * columns_here:(f + 1) * columns_here, :] = (
                feat[f, margin - 1] + gathered_columns(f, 0)
            )

    block = rep_size * rows
    for h in range(own_heads):
        arrived(qkv.at[h, :, pl.ds(0, others * rows), :], recv_sem.at[h])
        out_columns = pl.ds(pl.multiple_of((me * own_heads + h) * HEAD_DIM, HEAD_DIM), HEAD_DIM)

        def attend(step, carry):
            target = lax.rem(seq + 2 + step, seq_size)
            here = pl.ds(pl.multiple_of(target * block, block), block)
            scores = lax.dot_general(
                qkv[h, 0, here, :], qkv[h, 1], (((1,), (1,)), ((), ())),
                preferred_element_type=jnp.float32,
            ) * factor
            exponent = jnp.exp(scores - jnp.max(scores, axis=1, keepdims=True))
            total = jnp.sum(exponent, axis=1, keepdims=True)
            summed = jnp.dot(
                exponent.astype(jnp.bfloat16), qkv[h, 2], preferred_element_type=jnp.float32
            )
            obuf[h, here, :] = (summed / total).astype(jnp.bfloat16)
            for r in range(rep_size):
                @pl.when(jnp.logical_or(target != seq, rep != r))
                def _():
                    start = pl.multiple_of(target * block + r * rows, rows)
                    pltpu.make_async_remote_copy(
                        src_ref=obuf.at[h, pl.ds(start, rows), :],
                        dst_ref=att.at[:, out_columns],
                        send_sem=osend_sem,
                        recv_sem=orecv_sem.at[h],
                        device_id={"seq": target, "rep": r},
                        device_id_type=MESH,
                    ).start()
            return carry

        lax.fori_loop(0, seq_size, attend, 0)
        att[:, out_columns] = obuf[h, my_rows, :]
        if h == 0:
            last_layer()

    squares = jnp.zeros((rows, HEAD_DIM), jnp.float32)
    projected = jnp.zeros((rows, lw_ref.shape[0]), jnp.float32)
    for h in range(own_heads):
        arrived(obuf.at[h, pl.ds(0, others * rows), :], orecv_sem.at[h])
        for j in range(count):
            low = (j * own_heads + h) * HEAD_DIM
            cols = slice(low, low + HEAD_DIM)
            combined = stream_ref[:, cols].astype(jnp.float32) + att[:, cols].astype(jnp.float32)
            hidden = combined.astype(jnp.bfloat16)
            hid_ref[:, cols] = hidden
            widened = hidden.astype(jnp.float32)
            squares = squares + widened * widened
            scaled = (widened * gain_ref[:, cols]).astype(jnp.bfloat16)
            projected = projected + lax.dot_general(
                scaled, lw_ref[:, cols], (((1,), (1,)), ((), ())),
                preferred_element_type=jnp.float32,
            )
    latent = projected.shape[1]
    summed = jnp.sum(squares, axis=1, keepdims=True)
    part[:, :latent] = projected
    part[:, latent:] = jnp.broadcast_to(summed, (rows, part.shape[1] - latent))
    swap = pltpu.make_async_remote_copy(
        src_ref=part, dst_ref=part_in, send_sem=psend_sem, recv_sem=precv_sem,
        device_id=partner, device_id_type=MESH,
    )
    swap.start()
    arrived(qkv.at[:, :, pl.ds(0, others * rows), :], send_sem)
    arrived(obuf.at[:, pl.ds(0, others * rows), :], osend_sem)
    swap.wait()
    arrived(tiles.at[pl.ds(0, seq_size - 1), pl.ds(0, share), :], dsend_sem.at[0])
    arrived(lifts.at[pl.ds(0, pieces)], dsend_sem.at[1])
    arrived(biases.at[pl.ds(0, pieces)], dsend_sem.at[2])
    arrived(tiles.at[:, pl.ds(0, pieces * share), :], dsend_sem.at[3])
    arrived(act2.at[:, :, :, pl.ds(0, pieces * own)], dsend_sem.at[4])
    both = part[...] + part_in[...]
    width = q_ref.shape[1] * head_size
    lat_ref[...] = both[:, :latent] * lax.rsqrt(both[:, latent:latent + 1] / width + epsilon)


def fused(
    queries, key_tokens, value_tokens, stream, norm_gain, latent_weight,
    tile_pool, tile_position, lift_weight, lift_bias, conv_weight,
):
    seq_size, rep_size, head_size = (lax.axis_size(a) for a in ("seq", "rep", "head"))
    rows, width = queries.shape
    count = seq_size * rep_size
    own_heads = width // HEAD_DIM // count
    latent = latent_weight.shape[1]
    lanes = 2 * latent
    depth, frames, columns = tile_pool.shape[1:]
    layers, _, own, channels = conv_weight.shape
    quarters = head_size * rep_size
    reach = 2 * layers + 1
    bf = jnp.bfloat16
    vmem = pl.BlockSpec(memory_space=pltpu.VMEM)
    smem = pl.BlockSpec(memory_space=pltpu.SMEM)
    dma = pltpu.SemaphoreType.DMA
    grid_rows = lax.axis_index("seq") + jnp.arange(reach, dtype=jnp.int32) - layers
    pick = (grid_rows[:, None] == tile_position[None, :]).astype(jnp.float32)
    hidden, latents, decoded = pl.pallas_call(
        functools.partial(fused_kernel, seq_size, rep_size, head_size),
        out_shape=(
            jax.ShapeDtypeStruct((rows, width), bf),
            jax.ShapeDtypeStruct((rows, latent), jnp.float32),
            jax.ShapeDtypeStruct((frames * columns, own), jnp.float32),
        ),
        in_specs=[vmem] * 7 + [smem, vmem, vmem, pl.BlockSpec(memory_space=pl.ANY)],
        out_specs=(vmem, vmem, vmem),
        scratch_shapes=[
            pltpu.VMEM((own_heads, 3, count * rows, HEAD_DIM), bf),
            pltpu.VMEM((own_heads, count * rows, HEAD_DIM), bf),
            pltpu.VMEM((rows, width), bf),
            pltpu.VMEM((rows, lanes), jnp.float32),
            pltpu.VMEM((rows, lanes), jnp.float32),
            pltpu.VMEM((seq_size, depth, frames * columns), bf),
            pltpu.VMEM((quarters, depth, own), bf),
            pltpu.VMEM((quarters, 8, own), jnp.float32),
            pltpu.VMEM(conv_weight.shape, bf),
            pltpu.VMEM((frames, reach, columns, channels), bf),
            pltpu.VMEM((frames, reach - 2, columns, channels), bf),
            pltpu.VMEM((frames, reach - 2, columns, own), jnp.float32),
            pltpu.VMEM((frames, (reach - 2) * columns, 3 * own), jnp.float32),
            dma, dma((own_heads,)), dma, dma((own_heads,)), dma, dma,
            dma, dma((5,)), dma((5,)),
        ],
        compiler_params=pltpu.CompilerParams(
            collective_id=0, has_side_effects=True, vmem_limit_bytes=56 << 20
        ),
    )(
        queries, key_tokens, value_tokens, stream, norm_gain[None, :], latent_weight.T,
        tile_pool[0].reshape(depth, frames * columns), pick, lift_weight,
        jnp.broadcast_to(lift_bias[None, :], (8, own)), conv_weight,
    )
    decoded = decoded.reshape(frames, columns, own).transpose(2, 0, 1)[:, :, None, :]
    return hidden, latents, decoded


def gathered(queries, key_tokens, value_tokens, stream, norm_gain, latent_weight):
    query_heads, initial = prepare(queries)
    state = make_update(
        query_heads,
        initial,
        (
            lax.all_gather(key_tokens, ("seq", "rep"), axis=0, tiled=True),
            lax.all_gather(value_tokens, ("seq", "rep"), axis=0, tiled=True),
        ),
    )
    attended = finish(state)
    combined = stream.astype(jnp.float32) + attended.astype(jnp.float32)
    hidden = combined.astype(jnp.bfloat16)
    widened = hidden.astype(jnp.float32)
    scaled = (widened * norm_gain).astype(jnp.bfloat16)
    partial_proj = jnp.dot(scaled, latent_weight, preferred_element_type=jnp.float32)
    partial_squares = jnp.sum(widened * widened, axis=1)
    projected, squares = (
        lax.psum(partial_proj.astype(jnp.bfloat16), "head").astype(jnp.float32),
        lax.psum(partial_squares.astype(jnp.bfloat16), "head").astype(jnp.float32),
    )
    latents = projected * lax.rsqrt(squares / WIDTH + epsilon)[:, None]
    return hidden, latents


def shards(
    queries,
    key_tokens,
    value_tokens,
    stream,
    norm_gain,
    latent_weight,
    tile_pool,
    tile_position,
    lift_weight,
    lift_bias,
    conv_weight,
):
    heads_here = queries.shape[1] // HEAD_DIM
    spread = lax.axis_size("seq") * lax.axis_size("rep")
    fits = heads_here % spread == 0 and lax.axis_size("seq") == 4 and lax.axis_size("head") == 2
    fits = fits and lax.axis_size("rep") == 2 and tile_pool.shape[0] == 1
    fits = fits and conv_weight.shape[0] == 2 and lift_weight.shape[0] % 64 == 0
    if fits:
        return fused(
            queries, key_tokens, value_tokens, stream, norm_gain, latent_weight,
            tile_pool, tile_position, lift_weight, lift_bias, conv_weight,
        )
    hidden, latents = gathered(
        queries, key_tokens, value_tokens, stream, norm_gain, latent_weight
    )
    tiles_here = tile_pool.shape[0]
    frames = tile_pool.shape[2]
    columns = tile_pool.shape[3]
    own_rows = lax.axis_index("seq") * tiles_here + jnp.arange(tiles_here, dtype=jnp.int32)
    collected = make_pick(
        tile_position, own_rows, lax.all_gather(tile_pool, "seq", axis=0, tiled=True)
    )
    latent_grid = collected.astype(jnp.bfloat16)
    channels_here = lift_weight.shape[1]
    feature_map = (
        lax.dot_general(
            lift_weight,
            latent_grid.reshape(latent_grid.shape[0], -1),
            (((0,), (0,)), ((), ())),
            preferred_element_type=jnp.float32,
        )
        + lift_bias[:, None]
    )
    for layer_index in range(conv_weight.shape[0]):
        layer_weight = conv_weight[layer_index]
        active = (
            jax.nn.silu(feature_map)
            .astype(jnp.bfloat16)
            .reshape(channels_here, frames, tiles_here, columns)
        )
        zeros_here = jnp.zeros(feature_map.shape, jnp.float32)
        bordered = padded(active, (("seq", 2),), 1)
        rimmed = lax.all_gather(bordered, ("head", "rep"), axis=0, tiled=True)
        update = tap_sum(zeros_here, rimmed, layer_weight)
        feature_map = feature_map + update
    decoded = feature_map.reshape(channels_here, frames, tiles_here, columns)
    return (hidden, latents, decoded)


def solution(mesh):
    in_specs = (
        P(("groups", "seq", "rep"), "head"),
        P(("groups", "seq", "rep"), "head"),
        P(("groups", "seq", "rep"), "head"),
        P(("groups", "seq", "rep"), "head"),
        P("head"),
        P("head", None),
        P(("groups", "seq"), None, None, None),
        P("groups"),
        P(None, ("head", "rep")),
        P(("head", "rep")),
        P(None, None, ("head", "rep"), None),
    )
    out_specs = (
        P(("groups", "seq", "rep"), "head"),
        P(("groups", "seq", "rep"), None),
        P(("groups", "head", "rep"), None, "seq", None),
    )
    return jax.shard_map(shards, mesh=mesh, in_specs=in_specs, out_specs=out_specs, check_vma=False)
```

```python
import functools
import math

import jax
import jax.numpy as jnp
from jax import lax
from jax.experimental import pallas as pl
from jax.experimental.pallas import tpu as pltpu
from jax.sharding import PartitionSpec as P

HEAD_DIM = 128
WIDTH = 6144


epsilon = 1e-06
negative = -1e30


def padded(shard, sides, width):
    for axis, dim in sides:
        peers, length = (lax.axis_size(axis), shard.shape[dim])
        up = [(i, (i + 1) % peers) for i in range(peers - 1)]
        down = [(j, i) for i, j in up]
        last = lax.slice_in_dim(shard, length - width, length, axis=dim)
        leading = lax.slice_in_dim(shard, 0, width, axis=dim)
        before = lax.ppermute(last, axis, up)
        after = lax.ppermute(leading, axis, down)
        shard = jnp.concatenate([before, shard, after], axis=dim)
    return shard


def prepare(block_rows):
    row_count = block_rows.shape[0]
    head_count = block_rows.shape[1] // HEAD_DIM
    query_heads = block_rows.reshape(row_count, head_count, HEAD_DIM)
    initial = (
        jnp.full((head_count, row_count), negative, jnp.float32),
        jnp.zeros((head_count, row_count), jnp.float32),
        jnp.zeros((head_count, row_count, HEAD_DIM), jnp.float32),
    )
    return (query_heads, initial)


def make_update(query_heads, state, pieces):
    head_count = query_heads.shape[1]
    factor = 1.0 / math.sqrt(HEAD_DIM)
    running_max, running_sum, accum = state
    key_piece, value_piece = pieces
    piece_rows = key_piece.shape[0]
    key_heads = key_piece.reshape(piece_rows, head_count, HEAD_DIM)
    value_heads = value_piece.reshape(piece_rows, head_count, HEAD_DIM)
    scores = (
        jnp.einsum("qhd,khd->hqk", query_heads, key_heads, preferred_element_type=jnp.float32)
        * factor
    )
    new_max = jnp.maximum(running_max, jnp.max(scores, axis=2))
    exponent = jnp.exp(scores - new_max[:, :, None])
    running_sum = jnp.sum(exponent, axis=2)
    accum = jnp.einsum(
        "hqk,khd->hqd",
        exponent.astype(jnp.bfloat16),
        value_heads,
        preferred_element_type=jnp.float32,
    )
    return (new_max, running_sum, accum)


def finish(state):
    running_max, running_sum, accum = state
    result = accum / running_sum[:, :, None]
    return jnp.transpose(result, (1, 0, 2)).reshape(result.shape[1], -1).astype(jnp.bfloat16)


def shift_columns(window, col_shift):
    if col_shift == 0:
        return window
    edge = jnp.zeros(window.shape[:-1] + (1,), window.dtype)
    if col_shift < 0:
        return jnp.concatenate([edge, window[..., :-1]], axis=-1)
    return jnp.concatenate([window[..., 1:], edge], axis=-1)


def tap_sum(running, piece_block, layer_weight):
    piece_rows = piece_block.shape[0]
    frames = piece_block.shape[1]
    band_rows = piece_block.shape[2] - 2
    framed = jnp.pad(piece_block, ((0, 0), (1, 1), (0, 0), (0, 0)))
    for frame_off in range(3):
        for row_off in range(3):
            for col_off in range(3):
                window = shift_columns(
                    framed[:, frame_off : frame_off + frames, row_off : row_off + band_rows, :],
                    col_off - 1,
                )
                tap_weight = layer_weight[frame_off * 9 + row_off * 3 + col_off]
                running = running + lax.dot_general(
                    tap_weight,
                    window.reshape(piece_rows, -1),
                    (((1,), (0,)), ((), ())),
                    preferred_element_type=jnp.float32,
                )
    return running


def make_pick(tile_position, own_rows, piece_block):
    selector = (own_rows[:, None] == tile_position[None, :]).astype(jnp.bfloat16)
    return jnp.einsum("tp,plfc->lftc", selector, piece_block, preferred_element_type=jnp.float32)


MESH = pl.DeviceIdType.MESH


def fused_kernel(
    seq_size, rep_size, head_size,
    q_hbm, k_hbm, v_hbm, stream_hbm, gain_ref, lw_ref,
    tile_ref, place_ref, lift_ref, bias_ref, conv_ref,
    hid_hbm, sums_ref, dec_ref,
    q_ref, k_ref, v_ref, stream_ref, hid_ref,
    qkv, obuf, att, part, part_in,
    tiles, lifts, biases, taps, act1, act2, feat, acc,
    send_sem, recv_sem, osend_sem, orecv_sem, psend_sem, precv_sem,
    load_sem, hid_sem, tap_sem, dsend_sem, drecv_sem,
):
    loads = [
        pltpu.make_async_copy(source, target, load_sem.at[i])
        for i, (source, target) in enumerate(
            ((q_hbm, q_ref), (k_hbm, k_ref), (v_hbm, v_ref), (stream_hbm, stream_ref))
        )
    ]
    for load in loads:
        load.start()
    seq, rep, head = (lax.axis_index(a) for a in ("seq", "rep", "head"))
    count = seq_size * rep_size
    me = seq * rep_size + rep
    rows = q_ref.shape[0]
    own_heads = qkv.shape[0]
    others = count - 1
    factor = 1.0 / math.sqrt(HEAD_DIM)
    offsets = [(d, e) for d in (2, 1, 3, 0) for e in range(rep_size) if (d, e) != (0, 0)]

    def peer(d, e):
        return lax.rem(seq + d, seq_size), lax.rem(rep + e, rep_size)

    partner = {"head": lax.rem(head + 1, head_size)}
    mates = [
        {"head": lax.rem(head + d, head_size), "rep": lax.rem(rep + e, rep_size)}
        for d in range(head_size) for e in range(rep_size) if (d, e) != (0, 0)
    ]
    quarter = head * rep_size + rep
    tap_copy = pltpu.make_async_copy(conv_ref, taps, tap_sem)
    tap_copy.start()
    barrier = pltpu.get_barrier_semaphore()
    for d, e in offsets:
        ps, pr = peer(d, e)
        pl.semaphore_signal(barrier, inc=1, device_id={"seq": ps, "rep": pr}, device_id_type=MESH)
    strangers = [m for m, e in zip(mates, range(1, head_size * rep_size)) if e >= rep_size]
    for mate in strangers:
        pl.semaphore_signal(barrier, inc=1, device_id=mate, device_id_type=MESH)
    pl.semaphore_wait(barrier, others + len(strangers))

    def arrived(ref, sem):
        pltpu.make_async_copy(ref, ref, sem).wait()

    def send(source, target, index, device):
        pltpu.make_async_remote_copy(
            src_ref=source, dst_ref=target,
            send_sem=dsend_sem.at[index], recv_sem=drecv_sem.at[index],
            device_id=device, device_id_type=MESH,
        ).start()

    share = tile_ref.shape[1] // (head_size * rep_size)
    my_share = pl.ds(pl.multiple_of(quarter * share, share), share)
    for d in range(1, seq_size):
        send(tile_ref.at[0, my_share], tiles.at[seq, my_share], 0,
             {"seq": lax.rem(seq + d, seq_size)})
    for mate in mates:
        send(lift_ref, lifts.at[quarter], 1, mate)
        send(bias_ref, biases.at[quarter], 2, mate)

    for load in loads[:3]:
        load.wait()
    my_rows = pl.ds(pl.multiple_of(me * rows, rows), rows)
    sources = (q_ref, k_ref, v_ref)
    for h in range(own_heads):
        for d, e in offsets:
            ps, pr = peer(d, e)
            column = ((ps * rep_size + pr) * own_heads + h) * HEAD_DIM
            columns = pl.ds(pl.multiple_of(column, HEAD_DIM), HEAD_DIM)
            for a, source in enumerate(sources):
                pltpu.make_async_remote_copy(
                    src_ref=source.at[:, columns],
                    dst_ref=qkv.at[h, a, my_rows, :],
                    send_sem=send_sem,
                    recv_sem=recv_sem.at[h],
                    device_id={"seq": ps, "rep": pr},
                    device_id_type=MESH,
                ).start()
    for h in range(own_heads):
        columns = pl.ds(pl.multiple_of((me * own_heads + h) * HEAD_DIM, HEAD_DIM), HEAD_DIM)
        for a, source in enumerate(sources):
            qkv[h, a, my_rows, :] = source[:, columns]

    tiles[seq, my_share] = tile_ref[0, my_share]
    lifts[quarter] = lift_ref[...]
    biases[quarter] = bias_ref[...]
    pieces = len(mates)
    arrived(tiles.at[pl.ds(0, seq_size - 1), pl.ds(0, share)], drecv_sem.at[0])
    for mate in mates:
        send(tiles.at[:, my_share], tiles.at[:, my_share], 3, mate)
    arrived(lifts.at[pl.ds(0, pieces)], drecv_sem.at[1])
    arrived(biases.at[pl.ds(0, pieces)], drecv_sem.at[2])
    arrived(tiles.at[:, pl.ds(0, pieces * share)], drecv_sem.at[3])

    frames, reach, columns_here, channels = act1.shape
    own = lift_ref.shape[1]
    margin = reach // 2
    own_lanes = pl.ds(pl.multiple_of(quarter * own, own), own)

    def inside(d):
        row = seq + d
        return jnp.where(jnp.logical_and(row >= 0, row < seq_size), 1.0, 0.0)

    def silu(value):
        return value / (1.0 + jnp.exp(-value))

    def lifted(chosen, weight, bias):
        return lax.dot_general(
            chosen, weight, (((0,), (0,)), ((), ())), preferred_element_type=jnp.float32
        ) + bias

    wide = [tiles[p].astype(jnp.float32) for p in range(seq_size)]
    for d in range(reach):
        picked = jnp.zeros(wide[0].shape, jnp.float32)
        for p in range(seq_size):
            picked = picked + jnp.where(place_ref[p] == seq + d - margin, 1.0, 0.0) * wide[p]
        for f in range(frames):
            chosen = picked[:, f, :].astype(jnp.bfloat16)
            for c in range(pieces + 1):
                active = silu(lifted(chosen, lifts[c], biases[c])) * inside(d - margin)
                act1[f, d, :, c * own:(c + 1) * own] = active.astype(jnp.bfloat16)
            if 1 <= d <= reach - 2:
                feat[f, d - 1] = lifted(chosen, lift_ref[...], bias_ref[...])

    def convolve(layer, active, rows_out):
        length = rows_out * columns_here
        for f in range(frames):
            first = True
            for a in range(3):
                if not 0 <= f + a - 1 < frames:
                    continue
                for b in range(3):
                    window = active[f + a - 1, b:b + rows_out].reshape(length, channels)
                    base = 9 * a + 3 * b
                    term = lax.dot_general(
                        window, taps[layer, base:base + 3].reshape(3 * own, channels),
                        (((1,), (1,)), ((), ())), preferred_element_type=jnp.float32,
                    )
                    acc[f, :length, :] = term if first else acc[f, :length, :] + term
                    first = False

    def gathered_columns(f, r):
        lines = slice(r * columns_here, (r + 1) * columns_here)
        at = lax.broadcasted_iota(jnp.int32, (columns_here, own), 0)
        before = pltpu.roll(acc[f, lines, :own], 1, 0)
        after = pltpu.roll(acc[f, lines, 2 * own:], columns_here - 1, 0)
        return (
            acc[f, lines, own:2 * own]
            + jnp.where(at == 0, 0.0, before)
            + jnp.where(at == columns_here - 1, 0.0, after)
        )

    tap_copy.wait()
    convolve(0, act1, reach - 2)
    for f in range(frames):
        for r in range(reach - 2):
            value = feat[f, r] + gathered_columns(f, r)
            feat[f, r] = value
            act2[f, r, :, own_lanes] = (silu(value) * inside(r + 1 - margin)).astype(jnp.bfloat16)
    for mate in mates:
        send(act2.at[:, :, :, own_lanes], act2.at[:, :, :, own_lanes], 4, mate)

    def last_layer():
        arrived(act2.at[:, :, :, pl.ds(0, pieces * own)], drecv_sem.at[4])
        convolve(1, act2, reach - 4)
        for f in range(frames):
            dec_ref[f * columns_here:(f + 1) * columns_here, :] = (
                feat[f, margin - 1] + gathered_columns(f, 0)
            )

    block = rep_size * rows
    for h in range(own_heads):
        arrived(qkv.at[h, :, pl.ds(0, others * rows), :], recv_sem.at[h])
        out_columns = pl.ds(pl.multiple_of((me * own_heads + h) * HEAD_DIM, HEAD_DIM), HEAD_DIM)

        def attend(step, carry):
            target = lax.rem(seq + 2 + step, seq_size)
            here = pl.ds(pl.multiple_of(target * block, block), block)
            scores = lax.dot_general(
                qkv[h, 0, here, :], qkv[h, 1], (((1,), (1,)), ((), ())),
                preferred_element_type=jnp.float32,
            ) * factor
            exponent = jnp.exp(scores - jnp.max(scores, axis=1, keepdims=True))
            total = jnp.sum(exponent, axis=1, keepdims=True)
            summed = jnp.dot(
                exponent.astype(jnp.bfloat16), qkv[h, 2], preferred_element_type=jnp.float32
            )
            obuf[h, here, :] = (summed / total).astype(jnp.bfloat16)
            for r in range(rep_size):
                @pl.when(jnp.logical_or(target != seq, rep != r))
                def _():
                    start = pl.multiple_of(target * block + r * rows, rows)
                    pltpu.make_async_remote_copy(
                        src_ref=obuf.at[h, pl.ds(start, rows), :],
                        dst_ref=att.at[:, out_columns],
                        send_sem=osend_sem,
                        recv_sem=orecv_sem.at[h],
                        device_id={"seq": target, "rep": r},
                        device_id_type=MESH,
                    ).start()
            return carry

        lax.fori_loop(0, seq_size, attend, 0)
        att[:, out_columns] = obuf[h, my_rows, :]
        if h == 0:
            last_layer()

    loads[3].wait()
    squares = jnp.zeros((rows, HEAD_DIM), jnp.float32)
    projected = jnp.zeros((rows, lw_ref.shape[0]), jnp.float32)
    for h in range(own_heads):
        arrived(obuf.at[h, pl.ds(0, others * rows), :], orecv_sem.at[h])
        for j in range(count):
            low = (j * own_heads + h) * HEAD_DIM
            cols = slice(low, low + HEAD_DIM)
            combined = stream_ref[:, cols].astype(jnp.float32) + att[:, cols].astype(jnp.float32)
            hidden = combined.astype(jnp.bfloat16)
            hid_ref[:, cols] = hidden
            widened = hidden.astype(jnp.float32)
            squares = squares + widened * widened
            scaled = (widened * gain_ref[:, cols]).astype(jnp.bfloat16)
            projected = projected + lax.dot_general(
                scaled, lw_ref[:, cols], (((1,), (1,)), ((), ())),
                preferred_element_type=jnp.float32,
            )
    latent = projected.shape[1]
    summed = jnp.sum(squares, axis=1, keepdims=True)
    part[:, :latent] = projected
    part[:, latent:] = jnp.broadcast_to(summed, (rows, part.shape[1] - latent))
    swap = pltpu.make_async_remote_copy(
        src_ref=part, dst_ref=part_in, send_sem=psend_sem, recv_sem=precv_sem,
        device_id=partner, device_id_type=MESH,
    )
    swap.start()
    hid_copy = pltpu.make_async_copy(hid_ref, hid_hbm, hid_sem)
    hid_copy.start()
    arrived(qkv.at[:, :, pl.ds(0, others * rows), :], send_sem)
    arrived(obuf.at[:, pl.ds(0, others * rows), :], osend_sem)
    swap.wait()
    arrived(tiles.at[pl.ds(0, seq_size - 1), pl.ds(0, share)], dsend_sem.at[0])
    arrived(lifts.at[pl.ds(0, pieces)], dsend_sem.at[1])
    arrived(biases.at[pl.ds(0, pieces)], dsend_sem.at[2])
    arrived(tiles.at[:, pl.ds(0, pieces * share)], dsend_sem.at[3])
    arrived(act2.at[:, :, :, pl.ds(0, pieces * own)], dsend_sem.at[4])
    sums_ref[...] = part[...] + part_in[...]
    hid_copy.wait()


def finish_kernel(
    full_width, hid_in, sums_ref, dec_in, hid_out, lat_ref, dec_ref, held, in_sem, out_sem
):
    chunks = held.shape[0]
    size = hid_in.shape[0] // chunks
    reads = [
        pltpu.make_async_copy(hid_in.at[pl.ds(i * size, size), :], held.at[i], in_sem.at[i])
        for i in range(chunks)
    ]
    writes = [
        pltpu.make_async_copy(held.at[i], hid_out.at[pl.ds(i * size, size), :], out_sem.at[i])
        for i in range(chunks)
    ]
    for read in reads:
        read.start()
    for read, write in zip(reads, writes):
        read.wait()
        write.start()
    latent = lat_ref.shape[0]
    sums = jnp.transpose(sums_ref[...])
    lat_ref[...] = sums[:latent] * lax.rsqrt(sums[latent:latent + 1] / full_width + epsilon)
    frames = dec_ref.shape[0] // dec_in.shape[1]
    columns = dec_in.shape[0] // frames
    for f in range(frames):
        dec_ref[pl.ds(f, dec_in.shape[1], stride=frames), :] = jnp.transpose(
            dec_in[f * columns:(f + 1) * columns, :]
        )
    for write in writes:
        write.wait()


def fused(
    queries, key_tokens, value_tokens, stream, norm_gain, latent_weight,
    tile_pool, tile_position, lift_weight, lift_bias, conv_weight,
):
    seq_size, rep_size, head_size = (lax.axis_size(a) for a in ("seq", "rep", "head"))
    rows, width = queries.shape
    count = seq_size * rep_size
    own_heads = width // HEAD_DIM // count
    latent = latent_weight.shape[1]
    lanes = 2 * latent
    depth, frames, columns = tile_pool.shape[1:]
    layers, _, own, channels = conv_weight.shape
    quarters = head_size * rep_size
    reach = 2 * layers + 1
    bf = jnp.bfloat16
    vmem = pl.BlockSpec(memory_space=pltpu.VMEM)
    hbm = pl.BlockSpec(memory_space=pltpu.HBM)
    smem = pl.BlockSpec(memory_space=pltpu.SMEM)
    dma = pltpu.SemaphoreType.DMA
    hidden, sums, decoded = pl.pallas_call(
        functools.partial(fused_kernel, seq_size, rep_size, head_size),
        out_shape=(
            jax.ShapeDtypeStruct((rows, width), bf),
            jax.ShapeDtypeStruct((rows, lanes), jnp.float32),
            jax.ShapeDtypeStruct((frames * columns, own), jnp.float32),
        ),
        in_specs=[hbm] * 4 + [vmem] * 3 + [smem, vmem, vmem, hbm],
        out_specs=(hbm, vmem, vmem),
        scratch_shapes=[pltpu.VMEM((rows, width), bf)] * 5 + [
            pltpu.VMEM((own_heads, 3, count * rows, HEAD_DIM), bf),
            pltpu.VMEM((own_heads, count * rows, HEAD_DIM), bf),
            pltpu.VMEM((rows, width), bf),
            pltpu.VMEM((rows, lanes), jnp.float32),
            pltpu.VMEM((rows, lanes), jnp.float32),
            pltpu.VMEM((seq_size, depth, frames, columns), bf),
            pltpu.VMEM((quarters, depth, own), bf),
            pltpu.VMEM((quarters, 1, own), jnp.float32),
            pltpu.VMEM(conv_weight.shape, bf),
            pltpu.VMEM((frames, reach, columns, channels), bf),
            pltpu.VMEM((frames, reach - 2, columns, channels), bf),
            pltpu.VMEM((frames, reach - 2, columns, own), jnp.float32),
            pltpu.VMEM((frames, (reach - 2) * columns, 3 * own), jnp.float32),
            dma, dma((own_heads,)), dma, dma((own_heads,)), dma, dma,
            dma((4,)), dma, dma, dma((5,)), dma((5,)),
        ],
        compiler_params=pltpu.CompilerParams(
            collective_id=0, has_side_effects=True, vmem_limit_bytes=56 << 20
        ),
    )(
        queries, key_tokens, value_tokens, stream, norm_gain[None, :], latent_weight.T,
        tile_pool, tile_position, lift_weight, lift_bias[None, :], conv_weight,
    )
    chunks = 4
    hidden, latents, decoded = pl.pallas_call(
        functools.partial(finish_kernel, width * head_size),
        out_shape=(
            jax.ShapeDtypeStruct((rows, width), bf),
            jax.ShapeDtypeStruct((latent, rows), jnp.float32),
            jax.ShapeDtypeStruct((own * frames, columns), jnp.float32),
        ),
        in_specs=[hbm, vmem, vmem],
        out_specs=(hbm, vmem, vmem),
        scratch_shapes=[
            pltpu.VMEM((chunks, rows // chunks, width), bf), dma((chunks,)), dma((chunks,)),
        ],
    )(hidden, sums, decoded)
    return hidden, latents.T, decoded.reshape(own, frames, 1, columns)


def gathered(queries, key_tokens, value_tokens, stream, norm_gain, latent_weight):
    query_heads, initial = prepare(queries)
    state = make_update(
        query_heads,
        initial,
        (
            lax.all_gather(key_tokens, ("seq", "rep"), axis=0, tiled=True),
            lax.all_gather(value_tokens, ("seq", "rep"), axis=0, tiled=True),
        ),
    )
    attended = finish(state)
    combined = stream.astype(jnp.float32) + attended.astype(jnp.float32)
    hidden = combined.astype(jnp.bfloat16)
    widened = hidden.astype(jnp.float32)
    scaled = (widened * norm_gain).astype(jnp.bfloat16)
    partial_proj = jnp.dot(scaled, latent_weight, preferred_element_type=jnp.float32)
    partial_squares = jnp.sum(widened * widened, axis=1)
    projected, squares = (
        lax.psum(partial_proj.astype(jnp.bfloat16), "head").astype(jnp.float32),
        lax.psum(partial_squares.astype(jnp.bfloat16), "head").astype(jnp.float32),
    )
    latents = projected * lax.rsqrt(squares / WIDTH + epsilon)[:, None]
    return hidden, latents


def shards(
    queries,
    key_tokens,
    value_tokens,
    stream,
    norm_gain,
    latent_weight,
    tile_pool,
    tile_position,
    lift_weight,
    lift_bias,
    conv_weight,
):
    heads_here = queries.shape[1] // HEAD_DIM
    spread = lax.axis_size("seq") * lax.axis_size("rep")
    fits = heads_here % spread == 0 and lax.axis_size("seq") == 4 and lax.axis_size("head") == 2
    fits = fits and lax.axis_size("rep") == 2 and tile_pool.shape[0] == 1
    fits = fits and conv_weight.shape[0] == 2 and lift_weight.shape[0] % 64 == 0
    if fits:
        return fused(
            queries, key_tokens, value_tokens, stream, norm_gain, latent_weight,
            tile_pool, tile_position, lift_weight, lift_bias, conv_weight,
        )
    hidden, latents = gathered(
        queries, key_tokens, value_tokens, stream, norm_gain, latent_weight
    )
    tiles_here = tile_pool.shape[0]
    frames = tile_pool.shape[2]
    columns = tile_pool.shape[3]
    own_rows = lax.axis_index("seq") * tiles_here + jnp.arange(tiles_here, dtype=jnp.int32)
    collected = make_pick(
        tile_position, own_rows, lax.all_gather(tile_pool, "seq", axis=0, tiled=True)
    )
    latent_grid = collected.astype(jnp.bfloat16)
    channels_here = lift_weight.shape[1]
    feature_map = (
        lax.dot_general(
            lift_weight,
            latent_grid.reshape(latent_grid.shape[0], -1),
            (((0,), (0,)), ((), ())),
            preferred_element_type=jnp.float32,
        )
        + lift_bias[:, None]
    )
    for layer_index in range(conv_weight.shape[0]):
        layer_weight = conv_weight[layer_index]
        active = (
            jax.nn.silu(feature_map)
            .astype(jnp.bfloat16)
            .reshape(channels_here, frames, tiles_here, columns)
        )
        zeros_here = jnp.zeros(feature_map.shape, jnp.float32)
        bordered = padded(active, (("seq", 2),), 1)
        rimmed = lax.all_gather(bordered, ("head", "rep"), axis=0, tiled=True)
        update = tap_sum(zeros_here, rimmed, layer_weight)
        feature_map = feature_map + update
    decoded = feature_map.reshape(channels_here, frames, tiles_here, columns)
    return (hidden, latents, decoded)


def solution(mesh):
    in_specs = (
        P(("groups", "seq", "rep"), "head"),
        P(("groups", "seq", "rep"), "head"),
        P(("groups", "seq", "rep"), "head"),
        P(("groups", "seq", "rep"), "head"),
        P("head"),
        P("head", None),
        P(("groups", "seq"), None, None, None),
        P("groups"),
        P(None, ("head", "rep")),
        P(("head", "rep")),
        P(None, None, ("head", "rep"), None),
    )
    out_specs = (
        P(("groups", "seq", "rep"), "head"),
        P(("groups", "seq", "rep"), None),
        P(("groups", "head", "rep"), None, "seq", None),
    )
    return jax.shard_map(shards, mesh=mesh, in_specs=in_specs, out_specs=out_specs, check_vma=False)
```

```python
import functools
import math

import jax
import jax.numpy as jnp
from jax import lax
from jax.experimental import pallas as pl
from jax.experimental.pallas import tpu as pltpu
from jax.sharding import PartitionSpec as P

HEAD_DIM = 128
WIDTH = 6144


epsilon = 1e-06
negative = -1e30


def padded(shard, sides, width):
    for axis, dim in sides:
        peers, length = (lax.axis_size(axis), shard.shape[dim])
        up = [(i, (i + 1) % peers) for i in range(peers - 1)]
        down = [(j, i) for i, j in up]
        last = lax.slice_in_dim(shard, length - width, length, axis=dim)
        leading = lax.slice_in_dim(shard, 0, width, axis=dim)
        before = lax.ppermute(last, axis, up)
        after = lax.ppermute(leading, axis, down)
        shard = jnp.concatenate([before, shard, after], axis=dim)
    return shard


def prepare(block_rows):
    row_count = block_rows.shape[0]
    head_count = block_rows.shape[1] // HEAD_DIM
    query_heads = block_rows.reshape(row_count, head_count, HEAD_DIM)
    initial = (
        jnp.full((head_count, row_count), negative, jnp.float32),
        jnp.zeros((head_count, row_count), jnp.float32),
        jnp.zeros((head_count, row_count, HEAD_DIM), jnp.float32),
    )
    return (query_heads, initial)


def make_update(query_heads, state, pieces):
    head_count = query_heads.shape[1]
    factor = 1.0 / math.sqrt(HEAD_DIM)
    running_max, running_sum, accum = state
    key_piece, value_piece = pieces
    piece_rows = key_piece.shape[0]
    key_heads = key_piece.reshape(piece_rows, head_count, HEAD_DIM)
    value_heads = value_piece.reshape(piece_rows, head_count, HEAD_DIM)
    scores = (
        jnp.einsum("qhd,khd->hqk", query_heads, key_heads, preferred_element_type=jnp.float32)
        * factor
    )
    new_max = jnp.maximum(running_max, jnp.max(scores, axis=2))
    exponent = jnp.exp(scores - new_max[:, :, None])
    running_sum = jnp.sum(exponent, axis=2)
    accum = jnp.einsum(
        "hqk,khd->hqd",
        exponent.astype(jnp.bfloat16),
        value_heads,
        preferred_element_type=jnp.float32,
    )
    return (new_max, running_sum, accum)


def finish(state):
    running_max, running_sum, accum = state
    result = accum / running_sum[:, :, None]
    return jnp.transpose(result, (1, 0, 2)).reshape(result.shape[1], -1).astype(jnp.bfloat16)


def shift_columns(window, col_shift):
    if col_shift == 0:
        return window
    edge = jnp.zeros(window.shape[:-1] + (1,), window.dtype)
    if col_shift < 0:
        return jnp.concatenate([edge, window[..., :-1]], axis=-1)
    return jnp.concatenate([window[..., 1:], edge], axis=-1)


def tap_sum(running, piece_block, layer_weight):
    piece_rows = piece_block.shape[0]
    frames = piece_block.shape[1]
    band_rows = piece_block.shape[2] - 2
    framed = jnp.pad(piece_block, ((0, 0), (1, 1), (0, 0), (0, 0)))
    for frame_off in range(3):
        for row_off in range(3):
            for col_off in range(3):
                window = shift_columns(
                    framed[:, frame_off : frame_off + frames, row_off : row_off + band_rows, :],
                    col_off - 1,
                )
                tap_weight = layer_weight[frame_off * 9 + row_off * 3 + col_off]
                running = running + lax.dot_general(
                    tap_weight,
                    window.reshape(piece_rows, -1),
                    (((1,), (0,)), ((), ())),
                    preferred_element_type=jnp.float32,
                )
    return running


def make_pick(tile_position, own_rows, piece_block):
    selector = (own_rows[:, None] == tile_position[None, :]).astype(jnp.bfloat16)
    return jnp.einsum("tp,plfc->lftc", selector, piece_block, preferred_element_type=jnp.float32)


MESH = pl.DeviceIdType.MESH


def fused_kernel(
    seq_size, rep_size, head_size,
    q_hbm, k_hbm, v_hbm, stream_hbm, gain_ref, lw_ref,
    tile_ref, place_ref, lift_ref, bias_ref, conv_ref,
    hid_hbm, sums_ref, dec_ref,
    q_ref, k_ref, v_ref, stream_ref, hid_ref,
    qkv, obuf, att, part, part_in,
    tiles, lifts, biases, taps, act1, act2, feat, acc,
    send_sem, recv_sem, osend_sem, orecv_sem, psend_sem, precv_sem,
    load_sem, hid_sem, tap_sem, dsend_sem, drecv_sem,
):
    loads = [
        pltpu.make_async_copy(source, target, load_sem.at[i])
        for i, (source, target) in enumerate(
            ((q_hbm, q_ref), (k_hbm, k_ref), (v_hbm, v_ref), (stream_hbm, stream_ref))
        )
    ]
    for load in loads:
        load.start()
    seq, rep, head = (lax.axis_index(a) for a in ("seq", "rep", "head"))
    count = seq_size * rep_size
    me = seq * rep_size + rep
    rows = q_ref.shape[0]
    own_heads = qkv.shape[0]
    others = count - 1
    factor = 1.0 / math.sqrt(HEAD_DIM)
    offsets = [(d, e) for d in (2, 1, 3, 0) for e in range(rep_size) if (d, e) != (0, 0)]

    def peer(d, e):
        return lax.rem(seq + d, seq_size), lax.rem(rep + e, rep_size)

    partner = {"head": lax.rem(head + 1, head_size)}
    mates = [
        {"head": lax.rem(head + d, head_size), "rep": lax.rem(rep + e, rep_size)}
        for d in range(head_size) for e in range(rep_size) if (d, e) != (0, 0)
    ]
    quarter = head * rep_size + rep
    tap_copy = pltpu.make_async_copy(conv_ref, taps, tap_sem)
    tap_copy.start()
    barrier = pltpu.get_barrier_semaphore()
    for d, e in offsets:
        ps, pr = peer(d, e)
        pl.semaphore_signal(barrier, inc=1, device_id={"seq": ps, "rep": pr}, device_id_type=MESH)
    strangers = [m for m, e in zip(mates, range(1, head_size * rep_size)) if e >= rep_size]
    for mate in strangers:
        pl.semaphore_signal(barrier, inc=1, device_id=mate, device_id_type=MESH)
    pl.semaphore_wait(barrier, others + len(strangers))

    def arrived(ref, sem):
        pltpu.make_async_copy(ref, ref, sem).wait()

    def send(source, target, index, device):
        pltpu.make_async_remote_copy(
            src_ref=source, dst_ref=target,
            send_sem=dsend_sem.at[index], recv_sem=drecv_sem.at[index],
            device_id=device, device_id_type=MESH,
        ).start()

    share = tile_ref.shape[1] // (head_size * rep_size)
    my_share = pl.ds(pl.multiple_of(quarter * share, share), share)
    for d in range(1, seq_size):
        send(tile_ref.at[0, my_share], tiles.at[seq, my_share], 0,
             {"seq": lax.rem(seq + d, seq_size)})
    for mate in mates:
        send(lift_ref, lifts.at[quarter], 1, mate)
        send(bias_ref, biases.at[quarter], 2, mate)

    for load in loads[:3]:
        load.wait()
    my_rows = pl.ds(pl.multiple_of(me * rows, rows), rows)
    sources = (q_ref, k_ref, v_ref)
    for h in range(own_heads):
        for d, e in offsets:
            ps, pr = peer(d, e)
            column = ((ps * rep_size + pr) * own_heads + h) * HEAD_DIM
            columns = pl.ds(pl.multiple_of(column, HEAD_DIM), HEAD_DIM)
            for a, source in enumerate(sources):
                pltpu.make_async_remote_copy(
                    src_ref=source.at[:, columns],
                    dst_ref=qkv.at[h, a, my_rows, :],
                    send_sem=send_sem,
                    recv_sem=recv_sem.at[h],
                    device_id={"seq": ps, "rep": pr},
                    device_id_type=MESH,
                ).start()
    for h in range(own_heads):
        columns = pl.ds(pl.multiple_of((me * own_heads + h) * HEAD_DIM, HEAD_DIM), HEAD_DIM)
        for a, source in enumerate(sources):
            qkv[h, a, my_rows, :] = source[:, columns]

    tiles[seq, my_share] = tile_ref[0, my_share]
    lifts[quarter] = lift_ref[...]
    biases[quarter] = bias_ref[...]
    pieces = len(mates)
    arrived(tiles.at[pl.ds(0, seq_size - 1), pl.ds(0, share)], drecv_sem.at[0])
    for mate in mates:
        send(tiles.at[:, my_share], tiles.at[:, my_share], 3, mate)
    arrived(lifts.at[pl.ds(0, pieces)], drecv_sem.at[1])
    arrived(biases.at[pl.ds(0, pieces)], drecv_sem.at[2])
    arrived(tiles.at[:, pl.ds(0, pieces * share)], drecv_sem.at[3])

    frames, reach, columns_here, channels = act1.shape
    own = lift_ref.shape[1]
    margin = reach // 2
    own_lanes = pl.ds(pl.multiple_of(quarter * own, own), own)

    def inside(d):
        row = seq + d
        return jnp.where(jnp.logical_and(row >= 0, row < seq_size), 1.0, 0.0)

    def silu(value):
        return value / (1.0 + jnp.exp(-value))

    def lifted(chosen, weight, bias):
        return lax.dot_general(
            chosen, weight, (((0,), (0,)), ((), ())), preferred_element_type=jnp.float32
        ) + bias

    wide = [tiles[p].astype(jnp.float32) for p in range(seq_size)]
    for d in range(reach):
        picked = jnp.zeros(wide[0].shape, jnp.float32)
        for p in range(seq_size):
            picked = picked + jnp.where(place_ref[p] == seq + d - margin, 1.0, 0.0) * wide[p]
        for f in range(frames):
            chosen = picked[:, f, :].astype(jnp.bfloat16)
            for c in range(pieces + 1):
                active = silu(lifted(chosen, lifts[c], biases[c])) * inside(d - margin)
                act1[f, d, :, c * own:(c + 1) * own] = active.astype(jnp.bfloat16)
            if 1 <= d <= reach - 2:
                feat[f, d - 1] = lifted(chosen, lift_ref[...], bias_ref[...])

    def convolve(layer, active, rows_out):
        length = rows_out * columns_here
        for f in range(frames):
            first = True
            for a in range(3):
                if not 0 <= f + a - 1 < frames:
                    continue
                for b in range(3):
                    window = active[f + a - 1, b:b + rows_out].reshape(length, channels)
                    base = 9 * a + 3 * b
                    term = lax.dot_general(
                        window, taps[layer, base:base + 3].reshape(3 * own, channels),
                        (((1,), (1,)), ((), ())), preferred_element_type=jnp.float32,
                    )
                    acc[f, :length, :] = term if first else acc[f, :length, :] + term
                    first = False

    def gathered_columns(f, r):
        lines = slice(r * columns_here, (r + 1) * columns_here)
        at = lax.broadcasted_iota(jnp.int32, (columns_here, own), 0)
        before = pltpu.roll(acc[f, lines, :own], 1, 0)
        after = pltpu.roll(acc[f, lines, 2 * own:], columns_here - 1, 0)
        return (
            acc[f, lines, own:2 * own]
            + jnp.where(at == 0, 0.0, before)
            + jnp.where(at == columns_here - 1, 0.0, after)
        )

    tap_copy.wait()
    convolve(0, act1, reach - 2)
    for f in range(frames):
        for r in range(reach - 2):
            value = feat[f, r] + gathered_columns(f, r)
            feat[f, r] = value
            act2[f, r, :, own_lanes] = (silu(value) * inside(r + 1 - margin)).astype(jnp.bfloat16)
    for mate in mates:
        send(act2.at[:, :, :, own_lanes], act2.at[:, :, :, own_lanes], 4, mate)

    def last_layer():
        arrived(act2.at[:, :, :, pl.ds(0, pieces * own)], drecv_sem.at[4])
        convolve(1, act2, reach - 4)
        for f in range(frames):
            dec_ref[f * columns_here:(f + 1) * columns_here, :] = (
                feat[f, margin - 1] + gathered_columns(f, 0)
            )

    block = rep_size * rows
    for h in range(own_heads):
        arrived(qkv.at[h, :, pl.ds(0, others * rows), :], recv_sem.at[h])
        out_columns = pl.ds(pl.multiple_of((me * own_heads + h) * HEAD_DIM, HEAD_DIM), HEAD_DIM)

        def attend(step, carry):
            target = lax.rem(seq + 2 + step, seq_size)
            here = pl.ds(pl.multiple_of(target * block, block), block)
            scores = lax.dot_general(
                qkv[h, 0, here, :], qkv[h, 1], (((1,), (1,)), ((), ())),
                preferred_element_type=jnp.float32,
            ) * factor
            exponent = jnp.exp(scores - jnp.max(scores, axis=1, keepdims=True))
            total = jnp.sum(exponent, axis=1, keepdims=True)
            summed = jnp.dot(
                exponent.astype(jnp.bfloat16), qkv[h, 2], preferred_element_type=jnp.float32
            )
            obuf[h, here, :] = (summed / total).astype(jnp.bfloat16)
            for r in range(rep_size):
                @pl.when(jnp.logical_or(target != seq, rep != r))
                def _():
                    start = pl.multiple_of(target * block + r * rows, rows)
                    pltpu.make_async_remote_copy(
                        src_ref=obuf.at[h, pl.ds(start, rows), :],
                        dst_ref=att.at[:, out_columns],
                        send_sem=osend_sem,
                        recv_sem=orecv_sem.at[h],
                        device_id={"seq": target, "rep": r},
                        device_id_type=MESH,
                    ).start()
            return carry

        lax.fori_loop(0, seq_size, attend, 0)
        att[:, out_columns] = obuf[h, my_rows, :]
        if h == own_heads - 1:
            last_layer()

    loads[3].wait()
    squares = jnp.zeros((rows, HEAD_DIM), jnp.float32)
    projected = jnp.zeros((rows, lw_ref.shape[0]), jnp.float32)
    for h in range(own_heads):
        arrived(obuf.at[h, pl.ds(0, others * rows), :], orecv_sem.at[h])
        for j in range(count):
            low = (j * own_heads + h) * HEAD_DIM
            cols = slice(low, low + HEAD_DIM)
            combined = stream_ref[:, cols].astype(jnp.float32) + att[:, cols].astype(jnp.float32)
            hidden = combined.astype(jnp.bfloat16)
            hid_ref[:, cols] = hidden
            widened = hidden.astype(jnp.float32)
            squares = squares + widened * widened
            scaled = (widened * gain_ref[:, cols]).astype(jnp.bfloat16)
            projected = projected + lax.dot_general(
                scaled, lw_ref[:, cols], (((1,), (1,)), ((), ())),
                preferred_element_type=jnp.float32,
            )
    latent = projected.shape[1]
    summed = jnp.sum(squares, axis=1, keepdims=True)
    part[:, :latent] = projected
    part[:, latent:] = jnp.broadcast_to(summed, (rows, part.shape[1] - latent))
    swap = pltpu.make_async_remote_copy(
        src_ref=part, dst_ref=part_in, send_sem=psend_sem, recv_sem=precv_sem,
        device_id=partner, device_id_type=MESH,
    )
    swap.start()
    hid_copy = pltpu.make_async_copy(hid_ref, hid_hbm, hid_sem)
    hid_copy.start()
    arrived(qkv.at[:, :, pl.ds(0, others * rows), :], send_sem)
    arrived(obuf.at[:, pl.ds(0, others * rows), :], osend_sem)
    swap.wait()
    arrived(tiles.at[pl.ds(0, seq_size - 1), pl.ds(0, share)], dsend_sem.at[0])
    arrived(lifts.at[pl.ds(0, pieces)], dsend_sem.at[1])
    arrived(biases.at[pl.ds(0, pieces)], dsend_sem.at[2])
    arrived(tiles.at[:, pl.ds(0, pieces * share)], dsend_sem.at[3])
    arrived(act2.at[:, :, :, pl.ds(0, pieces * own)], dsend_sem.at[4])
    sums_ref[...] = part[...] + part_in[...]
    hid_copy.wait()


def finish_kernel(
    full_width, hid_in, sums_ref, dec_in, hid_out, lat_ref, dec_ref, held, in_sem, out_sem
):
    chunks = held.shape[0]
    size = hid_in.shape[0] // chunks
    reads = [
        pltpu.make_async_copy(hid_in.at[pl.ds(i * size, size), :], held.at[i], in_sem.at[i])
        for i in range(chunks)
    ]
    writes = [
        pltpu.make_async_copy(held.at[i], hid_out.at[pl.ds(i * size, size), :], out_sem.at[i])
        for i in range(chunks)
    ]
    for read in reads:
        read.start()
    for read, write in zip(reads, writes):
        read.wait()
        write.start()
    latent = lat_ref.shape[0]
    sums = jnp.transpose(sums_ref[...])
    lat_ref[...] = sums[:latent] * lax.rsqrt(sums[latent:latent + 1] / full_width + epsilon)
    frames = dec_ref.shape[0] // dec_in.shape[1]
    columns = dec_in.shape[0] // frames
    for f in range(frames):
        dec_ref[pl.ds(f, dec_in.shape[1], stride=frames), :] = jnp.transpose(
            dec_in[f * columns:(f + 1) * columns, :]
        )
    for write in writes:
        write.wait()


def fused(
    queries, key_tokens, value_tokens, stream, norm_gain, latent_weight,
    tile_pool, tile_position, lift_weight, lift_bias, conv_weight,
):
    seq_size, rep_size, head_size = (lax.axis_size(a) for a in ("seq", "rep", "head"))
    rows, width = queries.shape
    count = seq_size * rep_size
    own_heads = width // HEAD_DIM // count
    latent = latent_weight.shape[1]
    lanes = 2 * latent
    depth, frames, columns = tile_pool.shape[1:]
    layers, _, own, channels = conv_weight.shape
    quarters = head_size * rep_size
    reach = 2 * layers + 1
    bf = jnp.bfloat16
    vmem = pl.BlockSpec(memory_space=pltpu.VMEM)
    hbm = pl.BlockSpec(memory_space=pltpu.HBM)
    smem = pl.BlockSpec(memory_space=pltpu.SMEM)
    dma = pltpu.SemaphoreType.DMA
    hidden, sums, decoded = pl.pallas_call(
        functools.partial(fused_kernel, seq_size, rep_size, head_size),
        out_shape=(
            jax.ShapeDtypeStruct((rows, width), bf),
            jax.ShapeDtypeStruct((rows, lanes), jnp.float32),
            jax.ShapeDtypeStruct((frames * columns, own), jnp.float32),
        ),
        in_specs=[hbm] * 4 + [vmem] * 3 + [smem, vmem, vmem, hbm],
        out_specs=(hbm, vmem, vmem),
        scratch_shapes=[pltpu.VMEM((rows, width), bf)] * 5 + [
            pltpu.VMEM((own_heads, 3, count * rows, HEAD_DIM), bf),
            pltpu.VMEM((own_heads, count * rows, HEAD_DIM), bf),
            pltpu.VMEM((rows, width), bf),
            pltpu.VMEM((rows, lanes), jnp.float32),
            pltpu.VMEM((rows, lanes), jnp.float32),
            pltpu.VMEM((seq_size, depth, frames, columns), bf),
            pltpu.VMEM((quarters, depth, own), bf),
            pltpu.VMEM((quarters, 1, own), jnp.float32),
            pltpu.VMEM(conv_weight.shape, bf),
            pltpu.VMEM((frames, reach, columns, channels), bf),
            pltpu.VMEM((frames, reach - 2, columns, channels), bf),
            pltpu.VMEM((frames, reach - 2, columns, own), jnp.float32),
            pltpu.VMEM((frames, (reach - 2) * columns, 3 * own), jnp.float32),
            dma, dma((own_heads,)), dma, dma((own_heads,)), dma, dma,
            dma((4,)), dma, dma, dma((5,)), dma((5,)),
        ],
        compiler_params=pltpu.CompilerParams(
            collective_id=0, has_side_effects=True, vmem_limit_bytes=56 << 20
        ),
    )(
        queries, key_tokens, value_tokens, stream, norm_gain[None, :], latent_weight.T,
        tile_pool, tile_position, lift_weight, lift_bias[None, :], conv_weight,
    )
    chunks = 4
    hidden, latents, decoded = pl.pallas_call(
        functools.partial(finish_kernel, width * head_size),
        out_shape=(
            jax.ShapeDtypeStruct((rows, width), bf),
            jax.ShapeDtypeStruct((latent, rows), jnp.float32),
            jax.ShapeDtypeStruct((own * frames, columns), jnp.float32),
        ),
        in_specs=[hbm, vmem, vmem],
        out_specs=(hbm, vmem, vmem),
        scratch_shapes=[
            pltpu.VMEM((chunks, rows // chunks, width), bf), dma((chunks,)), dma((chunks,)),
        ],
    )(hidden, sums, decoded)
    return hidden, latents.T, decoded.reshape(own, frames, 1, columns)


def gathered(queries, key_tokens, value_tokens, stream, norm_gain, latent_weight):
    query_heads, initial = prepare(queries)
    state = make_update(
        query_heads,
        initial,
        (
            lax.all_gather(key_tokens, ("seq", "rep"), axis=0, tiled=True),
            lax.all_gather(value_tokens, ("seq", "rep"), axis=0, tiled=True),
        ),
    )
    attended = finish(state)
    combined = stream.astype(jnp.float32) + attended.astype(jnp.float32)
    hidden = combined.astype(jnp.bfloat16)
    widened = hidden.astype(jnp.float32)
    scaled = (widened * norm_gain).astype(jnp.bfloat16)
    partial_proj = jnp.dot(scaled, latent_weight, preferred_element_type=jnp.float32)
    partial_squares = jnp.sum(widened * widened, axis=1)
    projected, squares = (
        lax.psum(partial_proj.astype(jnp.bfloat16), "head").astype(jnp.float32),
        lax.psum(partial_squares.astype(jnp.bfloat16), "head").astype(jnp.float32),
    )
    latents = projected * lax.rsqrt(squares / WIDTH + epsilon)[:, None]
    return hidden, latents


def shards(
    queries,
    key_tokens,
    value_tokens,
    stream,
    norm_gain,
    latent_weight,
    tile_pool,
    tile_position,
    lift_weight,
    lift_bias,
    conv_weight,
):
    heads_here = queries.shape[1] // HEAD_DIM
    spread = lax.axis_size("seq") * lax.axis_size("rep")
    fits = heads_here % spread == 0 and lax.axis_size("seq") == 4 and lax.axis_size("head") == 2
    fits = fits and lax.axis_size("rep") == 2 and tile_pool.shape[0] == 1
    fits = fits and conv_weight.shape[0] == 2 and lift_weight.shape[0] % 64 == 0
    if fits:
        return fused(
            queries, key_tokens, value_tokens, stream, norm_gain, latent_weight,
            tile_pool, tile_position, lift_weight, lift_bias, conv_weight,
        )
    hidden, latents = gathered(
        queries, key_tokens, value_tokens, stream, norm_gain, latent_weight
    )
    tiles_here = tile_pool.shape[0]
    frames = tile_pool.shape[2]
    columns = tile_pool.shape[3]
    own_rows = lax.axis_index("seq") * tiles_here + jnp.arange(tiles_here, dtype=jnp.int32)
    collected = make_pick(
        tile_position, own_rows, lax.all_gather(tile_pool, "seq", axis=0, tiled=True)
    )
    latent_grid = collected.astype(jnp.bfloat16)
    channels_here = lift_weight.shape[1]
    feature_map = (
        lax.dot_general(
            lift_weight,
            latent_grid.reshape(latent_grid.shape[0], -1),
            (((0,), (0,)), ((), ())),
            preferred_element_type=jnp.float32,
        )
        + lift_bias[:, None]
    )
    for layer_index in range(conv_weight.shape[0]):
        layer_weight = conv_weight[layer_index]
        active = (
            jax.nn.silu(feature_map)
            .astype(jnp.bfloat16)
            .reshape(channels_here, frames, tiles_here, columns)
        )
        zeros_here = jnp.zeros(feature_map.shape, jnp.float32)
        bordered = padded(active, (("seq", 2),), 1)
        rimmed = lax.all_gather(bordered, ("head", "rep"), axis=0, tiled=True)
        update = tap_sum(zeros_here, rimmed, layer_weight)
        feature_map = feature_map + update
    decoded = feature_map.reshape(channels_here, frames, tiles_here, columns)
    return (hidden, latents, decoded)


def solution(mesh):
    in_specs = (
        P(("groups", "seq", "rep"), "head"),
        P(("groups", "seq", "rep"), "head"),
        P(("groups", "seq", "rep"), "head"),
        P(("groups", "seq", "rep"), "head"),
        P("head"),
        P("head", None),
        P(("groups", "seq"), None, None, None),
        P("groups"),
        P(None, ("head", "rep")),
        P(("head", "rep")),
        P(None, None, ("head", "rep"), None),
    )
    out_specs = (
        P(("groups", "seq", "rep"), "head"),
        P(("groups", "seq", "rep"), None),
        P(("groups", "head", "rep"), None, "seq", None),
    )
    return jax.shard_map(shards, mesh=mesh, in_specs=in_specs, out_specs=out_specs, check_vma=False)
```
